32 devices in a mesh: owner: 4 (over x, core), rows: 8 (over z, y).
Axes of the slice: x: 2, y: 2, z: 4, core: 2. Of those that a mesh axis runs over, the one named last changes fastest.
Arguments:
- train_gate: float32 [128, 2048, 768], P('owner', 'rows'), may hold values from -0.1875 to 0.1875
- train_up: float32 [128, 2048, 768], P('owner', 'rows'), may hold values from -0.1875 to 0.1875
- router_weight: float32 [2048, 128], P('rows', 'owner'), may hold values from -0.125 to 0.125
- router_gain: float32 [2048], P('rows'), may hold values from 0.25 to 1.75
Outputs:
- ready_gate: bfloat16 [128, 2048, 768], P(('owner', 'rows'))
- ready_up: bfloat16 [128, 2048, 768], P(('owner', 'rows'))
- scale_gate: float32 [128, 768], P(('owner', 'rows'))
- scale_up: float32 [128, 768], P(('owner', 'rows'))
- serve_router: bfloat16 [2048, 128], replicated
The draws below stay inside these ranges and needn't reach their ends.
All inputs are finite; a program needn't handle non-finite values.
Results may differ from the reference program's by a relative error of at most 0.001.
Values may be sent and summed in bfloat16 or wider, within the bound.
A program may use at most 192 MiB of HBM per device.

```python
import jax
import jax.numpy as jnp
from jax import lax

EXPERTS = 128
D_MODEL = 2048
D_EXPERT = 768


def spiked(drawn, rng, source, target, parts, factor):
    def block_of(position):
        return (jnp.arange(drawn.shape[position]) // (drawn.shape[position] // parts)).reshape((-1,) + (1,) * (drawn.ndim - 1 - position))

    near = jax.random.permutation(rng, parts)[block_of(target)]
    other_side = (block_of(target) + parts // 2) % parts
    return jnp.where((block_of(source) == near) | (block_of(source) == other_side), factor * drawn, drawn)


def shard_levels(key, dims, cuts, low, high):
    loudness, own = 1.0, jax.random.fold_in(key, 6)
    for axis_at, blocks in cuts:
        heights = jnp.exp(jax.random.uniform(jax.random.fold_in(own, axis_at), (blocks,), jnp.float32, low / len(cuts), high / len(cuts)))
        loudness = loudness * jnp.repeat(heights, dims[axis_at] // blocks).reshape([-1 if axis == axis_at else 1 for axis in range(len(dims))])
    return loudness


def noise(stream_key, extent, spread, most, split=(), dtype=jnp.bfloat16):
    result = jax.random.normal(stream_key, extent, jnp.float32) * spread
    if len(split) > 0:
        result = shard_levels(stream_key, extent, split, -0.22, 0.18) * result
    return jnp.clip(result, min=-most, max=most).astype(dtype)


def heavy_noise(stream_key, extent, spread, reach, pieces, heavy, kind=jnp.bfloat16):
    result = spread * jax.random.normal(stream_key, extent, jnp.float32)
    if pieces:
        result = result * shard_levels(stream_key, extent, pieces, -0.22, 0.18)
    return jnp.clip(spiked(result, jax.random.fold_in(stream_key, 3), *heavy), -reach, reach).astype(kind)


def setup_inputs(seed: int = 0) -> dict:
    splits = jax.random.split(jax.random.key(seed), 5)
    train_gate = heavy_noise(splits[0], (EXPERTS, D_MODEL, D_EXPERT), D_MODEL ** -0.5, 0.1875, ((0, 4), (1, 8)), (1, 2, 8, 2.0), jnp.float32)
    train_up = heavy_noise(splits[1], (EXPERTS, D_MODEL, D_EXPERT), D_MODEL ** -0.5, 0.1875, ((0, 4), (1, 8)), (1, 2, 8, 2.0), jnp.float32)
    router_weight = noise(splits[2], (D_MODEL, EXPERTS), D_MODEL ** -0.5, 0.125, ((0, 8), (1, 4)), jnp.float32)
    router_gain = jnp.clip(1.0 + 0.15 * jax.random.normal(splits[3], (D_MODEL,), jnp.float32), 0.25, 1.75)
    return dict(train_gate=train_gate, train_up=train_up, router_weight=router_weight, router_gain=router_gain)


def reference(train_gate, train_up, router_weight, router_gain):
    scale_gate = jnp.sqrt(lax.optimization_barrier(jnp.sum(train_gate * train_gate, axis=1)))
    ready_gate = (train_gate / jnp.expand_dims(scale_gate, 1)).astype(jnp.bfloat16)
    scale_up = jnp.sqrt(lax.optimization_barrier(jnp.sum(train_up * train_up, axis=1)))
    ready_up = (train_up / jnp.expand_dims(scale_up, 1)).astype(jnp.bfloat16)
    serve_router = (router_weight * router_gain[:, None]).astype(jnp.bfloat16)
    return (ready_gate, ready_up, scale_gate, scale_up, serve_router)
```

```python
import functools

import jax
import jax.numpy as jnp
from jax import lax
from jax.experimental import pallas as pl
from jax.experimental.pallas import tpu as pltpu
from jax.sharding import PartitionSpec as P

MESH = pl.DeviceIdType.MESH
CHUNK = 32


def pairing(n, me, k):
    if n & (n - 1):
        return lax.rem(me + k, n), lax.rem(me + n - k, n)
    other, bit = 0, 1
    while bit < n:
        own = (me // bit) % 2
        other = other + bit * ((1 - own) if k & bit else own)
        bit *= 2
    return other, other


def kernel(
    rows_n, owners_n,
    gate, up, weight, gain,
    ready_gate, ready_up, scale, router,
    slabs, send, part, gathered, scales, mine,
    load_sem, data_send, data_recv, sum_send, sum_recv, scale_send, scale_recv,
    own_sem, router_send, router_recv, router_own, forward_send, forward_recv,
):
    me, group = lax.axis_index("rows"), lax.axis_index("owner")
    height, width = gate.shape[2], gate.shape[3]
    each = gate.shape[1]
    steps = 2 * each
    far_first = list(range(rows_n - 1, -1, -1))
    place = [pairing(rows_n, me, k) for k in range(rows_n)]
    here = pl.ds(pl.multiple_of(me * height, height), height)

    def load(step, slab):
        bank, c = (gate, up)[step // each], step % each
        return [
            pltpu.make_async_copy(bank.at[place[k][0], c], slabs.at[slab, k], load_sem.at[slab, k])
            for k in range(rows_n)
        ]

    def begin(copies):
        for copy in copies:
            copy.start()

    def sum_one(slab, k, step):
        def add(i, total):
            x = slabs[slab, k, pl.ds(i * CHUNK, CHUNK), :]
            return total + jnp.sum((x * x).reshape(CHUNK // 8, 8, width), axis=0)

        total = lax.fori_loop(0, height // CHUNK, add, jnp.zeros((8, width), jnp.float32))
        part[place[k][0], step] = jnp.sum(total, axis=0, keepdims=True)

    def sum_copies(which, lo, hi):
        return [
            pltpu.make_async_remote_copy(
                part.at[place[k][0], pl.ds(lo, hi - lo)],
                gathered.at[me, pl.ds(lo, hi - lo)],
                sum_send.at[which, k], sum_recv.at[which, k],
                device_id={"rows": place[k][0]}, device_id_type=MESH,
            )
            for k in far_first[:-1]
        ]

    def scale_copies(which, lo, hi):
        return [
            pltpu.make_async_remote_copy(
                scales.at[me, pl.ds(lo, hi - lo)],
                scales.at[me, pl.ds(lo, hi - lo)],
                scale_send.at[which, k], scale_recv.at[which, k],
                device_id={"rows": place[k][0]}, device_id_type=MESH,
            )
            for k in far_first[:-1]
        ]

    def finish_sums(lo, hi):
        for step in range(lo, hi):
            gathered[me, step] = part[me, step]
        for step in range(lo, hi):
            total = gathered[0, step]
            for source in range(1, rows_n):
                total = total + gathered[source, step]
            root = jnp.sqrt(total)
            scales[me, step] = root
            scale[step] = root

    def data_copy(step, k):
        bank, c = (ready_gate, ready_up)[step // each], step % each
        if k == 0:
            return pltpu.make_async_copy(send.at[step, 0], bank.at[c, here], own_sem.at[step])
        return pltpu.make_async_remote_copy(
            send.at[step, k], bank.at[c, here], data_send.at[step, k], data_recv.at[step, k],
            device_id={"rows": place[k][0]}, device_id_type=MESH,
        )

    def ship(slab, k, step):
        by = scales[place[k][0], step]

        def narrow(i, carry):
            at = pl.ds(i * CHUNK, CHUNK)
            send[step, k, at, :] = (slabs[slab, k, at, :] / by).astype(jnp.bfloat16)
            return carry

        lax.fori_loop(0, height // CHUNK, narrow, 0)
        data_copy(step, k).start()

    first, second = load(0, 0), load(1, 1)
    begin([first[k] for k in far_first])
    begin([second[k] for k in far_first])

    barrier = pltpu.get_barrier_semaphore()
    for k in range(1, rows_n):
        pl.semaphore_signal(barrier, inc=1, device_id={"rows": place[k][0]}, device_id_type=MESH)
    for j in range(1, owners_n):
        pl.semaphore_signal(
            barrier, inc=1, device_id={"owner": lax.rem(group + j, owners_n)}, device_id_type=MESH
        )

    mine[...] = (weight[...] * gain[...]).astype(jnp.bfloat16)

    for k in far_first:
        first[k].wait()
        sum_one(0, k, 0)
    pl.semaphore_wait(barrier, rows_n + owners_n - 2)
    first_sums = sum_copies(0, 0, 1)
    begin(first_sums)
    for copy in first_sums:
        copy.wait_recv()
    finish_sums(0, 1)
    first_scales = scale_copies(0, 0, 1)
    begin(first_scales)
    for copy in first_scales:
        copy.wait_recv()

    lots = far_first[: rows_n // 4], far_first[rows_n // 4 : rows_n // 4 + rows_n // 8], far_first[rows_n // 4 + rows_n // 8 :]
    for k in lots[0]:
        ship(0, k, 0)

    columns = pl.ds(pl.multiple_of(me * height, height), height)
    router_copies = [
        pltpu.make_async_remote_copy(
            mine, router.at[group, :, columns], router_send.at[k], router_recv.at[k],
            device_id={"rows": place[k][0]}, device_id_type=MESH,
        )
        for k in far_first[:-1]
    ]
    router_local = pltpu.make_async_copy(mine, router.at[group, :, columns], router_own)
    router_local.start()

    waiting = second
    for step in range(1, steps):
        slab = 1 + (step - 1) % 2
        now = waiting
        if step + 1 < steps:
            waiting = load(step + 1, 1 + step % 2)
            begin(waiting)
        for k in range(rows_n):
            now[k].wait()
            sum_one(slab, k, step)
    rest_sums = sum_copies(1, 1, steps)
    begin(rest_sums)
    begin(router_copies)
    waiting = load(1, 1)
    begin(waiting)
    for k in lots[1]:
        ship(0, k, 0)
    for copy in rest_sums:
        copy.wait_recv()
    finish_sums(1, steps)
    rest_scales = scale_copies(1, 1, steps)
    begin(rest_scales)
    for k in lots[2]:
        ship(0, k, 0)
    for copy in rest_scales:
        copy.wait_recv()

    for step in range(1, steps):
        slab = 1 + (step - 1) % 2
        now = waiting
        if step + 1 < steps:
            waiting = load(step + 1, 1 + step % 2)
            begin(waiting)
        for k in far_first:
            now[k].wait()
            ship(slab, k, step)

    for copy in router_copies:
        copy.wait_recv()
    router_local.wait()
    forwards = []
    for j in range(1, owners_n):
        forwards.append(
            pltpu.make_async_remote_copy(
                router.at[group], router.at[group], forward_send.at[j], forward_recv.at[j],
                device_id={"owner": lax.rem(group + j, owners_n)}, device_id_type=MESH,
            )
        )
    begin(forwards)

    for copies in (first_sums, first_scales, rest_sums, rest_scales, router_copies):
        for copy in copies:
            copy.wait_send()
    for copy in forwards:
        copy.wait()
    for step in range(steps):
        for k in far_first:
            data_copy(step, k).wait()


def on_device(rows_n, owners_n, train_gate, train_up, router_weight, router_gain):
    experts, height, width = train_gate.shape
    each = experts // rows_n
    steps = 2 * each
    cols = router_weight.shape[1]
    f32, bf16, dma = jnp.float32, jnp.bfloat16, pltpu.SemaphoreType.DMA
    hbm, vmem = pl.BlockSpec(memory_space=pl.ANY), pl.BlockSpec(memory_space=pltpu.VMEM)
    ready = jax.ShapeDtypeStruct((each, rows_n * height, width), bf16)
    ready_gate, ready_up, scale, router = pl.pallas_call(
        functools.partial(kernel, rows_n, owners_n),
        out_shape=(
            ready,
            ready,
            jax.ShapeDtypeStruct((steps, 1, width), f32),
            jax.ShapeDtypeStruct((owners_n, cols, rows_n * height), bf16),
        ),
        in_specs=[hbm, hbm, vmem, vmem],
        out_specs=(hbm, hbm, vmem, hbm),
        scratch_shapes=[
            pltpu.VMEM((3, rows_n, height, width), f32),
            pltpu.VMEM((steps, rows_n, height, width), bf16),
            pltpu.VMEM((rows_n, steps, 1, width), f32),
            pltpu.VMEM((rows_n, steps, 1, width), f32),
            pltpu.VMEM((rows_n, steps, 1, width), f32),
            pltpu.VMEM((cols, height), bf16),
            dma((3, rows_n)),
            dma((steps, rows_n)),
            dma((steps, rows_n)),
            dma((2, rows_n)),
            dma((2, rows_n)),
            dma((2, rows_n)),
            dma((2, rows_n)),
            dma((steps,)),
            dma((rows_n,)),
            dma((rows_n,)),
            dma,
            dma((owners_n,)),
            dma((owners_n,)),
        ],
        compiler_params=pltpu.CompilerParams(
            collective_id=0, has_side_effects=True, vmem_limit_bytes=60 * 1024 * 1024
        ),
        name="serve",
    )(
        train_gate.reshape(rows_n, each, height, width),
        train_up.reshape(rows_n, each, height, width),
        router_weight.T,
        router_gain[None, :],
    )
    serve_router = router.reshape(owners_n * cols, rows_n * height).T
    scale = scale.reshape(steps, width)
    return (ready_gate, ready_up, scale[:each], scale[each:], serve_router)


def solution(mesh):
    return jax.shard_map(
        functools.partial(on_device, mesh.shape["rows"], mesh.shape["owner"]),
        mesh=mesh,
        in_specs=(
            P("owner", "rows", None),
            P("owner", "rows", None),
            P("rows", "owner"),
            P("rows"),
        ),
        out_specs=(
            P(("owner", "rows"), None, None),
            P(("owner", "rows"), None, None),
            P(("owner", "rows"), None),
            P(("owner", "rows"), None),
            P(),
        ),
        check_vma=False,
    )
```
